32 devices in a mesh: group: 2 (over x), seq: 16 (over z, y, core).
Axes of the slice: x: 2, y: 2, z: 4, core: 2. Of those that a mesh axis runs over, the one named last changes fastest.
Arguments:
- tokens: bfloat16 [16384, 4096], P(('group', 'seq')), parts along dimension 0, may hold values from -6 to 6
- norm_gain: bfloat16 [4096], replicated, may hold values from 0.099609375 to 1.8984375
- w_key: bfloat16 [4096, 1024], P('seq'), may hold values from -0.09375 to 0.09375
- w_value: bfloat16 [4096, 1024], P('seq'), may hold values from -0.09375 to 0.09375
- lengths: int32 [4], P('group'), parts along dimension 0, may hold values from 2048 to 4096
- page_table: int32 [1024], P(('group', 'seq')), parts along dimension 0, may hold values from 0 to 639, as said below
Outputs:
- kv_cache: bfloat16 [2, 1280, 16, 1024], P(None, ('group', 'seq')), parts along dimension 1
The draws below stay inside these ranges and needn't reach their ends.
There are 2 independent parts, one for each index of `group`. The reference program is written for one: setup_inputs(seed, part) draws one part's arguments, and reference() takes and returns one part's arrays. A program takes and returns all parts, laid end to end along the dimension named above; an argument that names none is the same for every part. Nothing has to cross between parts.
Inputs may be any that keep to these rules, and one draw needn't show every extreme that they name: The entries are distinct. Page g of the 32 pages of device s goes to slot page_table[g] of decode device page_table[g] // 40, which is s + k modulo 16 for an offset k in -2 .. 2, at a slot of the block of 8 slots from (k + 2) * 8 on; so at most 8 pages go from one device to one decode device, and exactly 8 from every device to some decode device.
All inputs are finite; a program needn't handle non-finite values.
Results may differ from the reference program's by a relative error of at most 0.0049.
Values may be sent and summed in bfloat16 or wider, within the bound.
No kernel may reach another device: no remote copies, remote signals or barrier semaphores. Data moves between devices by JAX's collectives and lax.ppermute only.
A program may use at most 64 MiB of HBM per device.

```python
import jax
import jax.numpy as jnp
from jax import lax

D = 4096
HEAD = 128
PAGE = 16
REACH = 2
TOK_DEV = 512
KVD = 1024
TOKENS = 8192
LENGTH = 4096
CAP = 8
SLOTS = 40
PAGES = 512
N_SEQ = 16


def draw_page_table(key, part):
    pages_dev = TOK_DEV // PAGE
    regions = 2 * REACH + 1

    def one_device(device):
        device_key = jax.random.fold_in(jax.random.fold_in(key, 7), device)
        first_key, second_key, third_key = jax.random.split(device_key, 3)
        full_region = jax.random.randint(first_key, (), 0, regions)
        ranks = jax.random.permutation(second_key, SLOTS)
        region_of = jnp.arange(SLOTS, dtype=jnp.int32) // CAP
        score = jnp.where(region_of == full_region, 0, SLOTS) + ranks
        order = jnp.argsort(score, stable=True)
        chosen = jax.random.permutation(third_key, order[:pages_dev])
        offset = chosen // CAP - REACH
        target = (device + offset) % N_SEQ
        return (target * SLOTS + chosen).astype(jnp.int32)
    table = jax.vmap(one_device)(jnp.arange(N_SEQ, dtype=jnp.int32))
    return table.reshape(-1).astype(jnp.int32)


def block_levels(key, shape, shards, low, top_value):
    factor_of = 1.0
    for axis_at, parts in shards:
        heights = jax.random.uniform(jax.random.fold_in(jax.random.fold_in(key, 6), axis_at), (parts,), jnp.float32, low / len(shards), top_value / len(shards))
        factor_of = factor_of * jnp.repeat(jnp.exp(heights), shape[axis_at] // parts).reshape((-1,) + (1,) * (len(shape) - 1 - axis_at))
    return factor_of


def bell_draw(own_key, extent, spread, most, cuts=(), kind=jnp.bfloat16):
    values = jax.random.normal(own_key, extent, jnp.float32) * spread
    if len(cuts) > 0:
        values = block_levels(own_key, extent, cuts, -0.22, 0.18) * values
    return jnp.clip(values, min=-most, max=most).astype(kind)


def setup_inputs(seed: int = 0, part: int = 0) -> dict:
    key_list = jax.random.split(jax.random.key(seed), 7)
    part_splits = jax.random.split(jax.random.fold_in(key_list[6], part), 7)
    return {
        "tokens": bell_draw(part_splits[0], (TOKENS, D), 1.0, 6.0, ((0, 16),)),
        "norm_gain": jnp.clip(1.0 + 0.18 * jax.random.normal(key_list[1], (D,), jnp.float32), 0.099609375, 1.8984375).astype(jnp.bfloat16),
        "w_key": bell_draw(key_list[2], (D, KVD), D ** -0.5, 0.09375, ((0, 16),)),
        "w_value": bell_draw(key_list[3], (D, KVD), D ** -0.5, 0.09375, ((0, 16),)),
        "lengths": jax.random.randint(part_splits[4], (2,), LENGTH // 2, LENGTH + 1).astype(jnp.int32),
        "page_table": draw_page_table(jax.random.fold_in(jax.random.fold_in(key_list[6], part), 71), part),
    }


ROPE_THETA = 500000.0
EPS = 1e-05

def rotate_keys(key_rows, position):
    half = HEAD // 2
    freq = ROPE_THETA ** (-(jnp.arange(half, dtype=jnp.float32) * 2.0 / HEAD))
    angle = position.astype(jnp.float32)[:, None] * freq[None, :]
    cosine = jnp.cos(angle)[:, None, :]
    sine = jnp.sin(angle)[:, None, :]
    shaped = key_rows.reshape(key_rows.shape[0], -1, HEAD)
    first = shaped[:, :, :half]
    second = shaped[:, :, half:]
    turned = jnp.concatenate([first * cosine - second * sine, second * cosine + first * sine], axis=2)
    return turned.reshape(key_rows.shape)

def reference(tokens, norm_gain, w_key, w_value, lengths, page_table):
    wide = tokens.astype(jnp.float32)
    scale = lax.rsqrt(lax.optimization_barrier(jnp.mean(wide * wide, axis=1, keepdims=True)) + EPS)
    normed = (wide * scale * norm_gain.astype(jnp.float32)[None, :]).astype(jnp.bfloat16)
    key_rows = jnp.dot(normed, w_key, preferred_element_type=jnp.float32)
    value_rows = jnp.dot(normed, w_value, preferred_element_type=jnp.float32)
    token_index = jnp.arange(TOKENS, dtype=jnp.int32)
    prompt_id = token_index // LENGTH
    position = token_index % LENGTH
    limit = jnp.where(prompt_id == 0, lengths[0], lengths[1])
    inside = (position < limit)[:, None]
    key_rows = rotate_keys(key_rows, position)
    keys = jnp.where(inside, key_rows, 0.0).astype(jnp.bfloat16)
    values = jnp.where(inside, value_rows, 0.0).astype(jnp.bfloat16)
    pages = jnp.stack([keys, values]).reshape(2, PAGES, PAGE, KVD)
    cache = jnp.zeros((2, N_SEQ * SLOTS, PAGE, KVD), jnp.bfloat16)
    return cache.at[:, page_table.astype(jnp.int32)].set(pages)
```

```python
import functools

import jax
import jax.numpy as jnp
from jax import lax
from jax.experimental import pallas as pl
from jax.experimental.pallas import tpu as pltpu
from jax.sharding import PartitionSpec as P


HEAD = 128
PAGE = 16
REACH = 2
CAP = 8
SLOTS = 40
CORES = 2
LANES = 128


ROPE_THETA = 500000.0
EPS = 1e-05


def shifted(block, axis, distance):
    devices = range(lax.axis_size(axis))
    route = [((i - distance) % len(devices), i) for i in devices]
    return lax.ppermute(block, axis, route)


def swapped(block, axis):
    return lax.ppermute(block, axis, [(i ^ 1, i) for i in range(lax.axis_size(axis))])


def grid_of(axis_size):
    chips = axis_size // CORES
    inner = 1 << ((chips.bit_length() - 1) // 2)
    return chips // inner, inner


def sent(block, outer_step, inner_step):
    axis_size = lax.axis_size("seq")
    outer, inner = grid_of(axis_size)
    route = []
    for i in range(axis_size):
        chip, core = divmod(i, CORES)
        row, column = divmod(chip, inner)
        to = (row + outer_step) % outer * inner + (column + inner_step) % inner
        route.append((i, to * CORES + core))
    return lax.ppermute(block, "seq", route)


def arrival_order():
    groups = lax.axis_size("group")
    group = lax.axis_index("group")
    outer, inner = grid_of(lax.axis_size("seq"))
    chip = lax.axis_index("seq") // CORES
    row, column = chip // inner, chip % inner

    def at(row_back, column_back, owner):
        place = (row - row_back + outer) % outer * inner + (column - column_back + inner) % inner
        return place, owner

    order = [at(0, 0, owner) for owner in range(groups)]
    order += [at(1, 0, owner) for owner in range(groups)]
    order += [at(0, step, owner) for step in range(1, inner) for owner in range(groups)]
    for turn in range(groups):
        owner = (group - turn + groups) % groups
        order += [at(step, 0, owner) for step in range(2, outer)]
        order += [
            at(back, step, owner) for step in range(1, inner) for back in range(1, outer)
        ]
    return order


def opened(shard):
    groups = lax.axis_size("group")
    group = lax.axis_index("group")
    outer, inner = grid_of(lax.axis_size("seq"))
    part = shard.shape[0] // groups
    columns = shard.shape[1]
    own = shard.reshape(groups, part, columns)

    def pick(blocks):
        return lax.dynamic_slice(blocks, (group, 0, 0), (1, part, columns))

    first = pick(own)
    far, across = [], []
    for step in range(2, outer):
        far.append(sent(first, step, 0))
    for step in range(1, inner):
        across.append(sent(own, 0, step))
    near = sent(own, 1, 0)
    rest = jnp.concatenate([pick(near)] + far, axis=0)
    return [own, near] + across, far, rest


def crossed(rest):
    crossing = []
    for step in range(1, grid_of(lax.axis_size("seq"))[1]):
        crossing.append(sent(rest, 0, step))
    return jnp.concatenate(crossing, axis=0)


def exchanged(whole, far, late):
    groups = lax.axis_size("group")
    early = jnp.concatenate(far, axis=0)
    gathered = whole + [early, late]
    for turn in range(1, groups):
        swap = [(i, (i + turn) % groups) for i in range(groups)]
        gathered.append(lax.ppermute(early, "group", swap))
        gathered.append(lax.ppermute(late, "group", swap))
    return [blocks.reshape(-1, blocks.shape[2]) for blocks in gathered]


def split_body(part, table, tokens_ref, gain_ref, mine_ref, other_ref, normed_ref):
    wide = tokens_ref[...].astype(jnp.float32)
    scale = lax.rsqrt(jnp.mean(wide * wide, axis=1, keepdims=True) + EPS)
    normed_ref[...] = (wide * scale * gain_ref[...].astype(jnp.float32)).astype(jnp.bfloat16)
    for which, out_ref in enumerate((mine_ref, other_ref)):
        for k in range(out_ref.shape[1] // part):
            start = pl.multiple_of(table[which, k] * part, part)
            out_ref[:, k * part : (k + 1) * part] = normed_ref[:, pl.ds(start, part)]


def normalised(tokens, norm_gain, table, part):
    rows, width = tokens.shape
    if part % LANES:
        wide = tokens.astype(jnp.float32)
        scale = lax.rsqrt(jnp.mean(wide * wide, axis=1, keepdims=True) + EPS)
        normed = (wide * scale * norm_gain.astype(jnp.float32)[None, :]).astype(jnp.bfloat16)
        blocks = normed.reshape(rows, width // part, part)
        return [jnp.take(blocks, table[which], axis=1).reshape(rows, -1) for which in range(2)]
    tile = min(rows, 64)
    half = jax.ShapeDtypeStruct((rows, width // CORES), jnp.bfloat16)
    row_block = pl.BlockSpec((tile, width // CORES), lambda i, table: (i, 0))
    return pl.pallas_call(
        functools.partial(split_body, part),
        grid_spec=pltpu.PrefetchScalarGridSpec(
            num_scalar_prefetch=1,
            grid=(rows // tile,),
            in_specs=[
                pl.BlockSpec((tile, width), lambda i, table: (i, 0)),
                pl.BlockSpec((1, width), lambda i, table: (0, 0)),
            ],
            out_specs=[row_block, row_block],
            scratch_shapes=[pltpu.VMEM((tile, width), jnp.bfloat16)],
        ),
        out_shape=[half, half],
        cost_estimate=pl.CostEstimate(
            flops=rows * width * 100, bytes_accessed=rows * width * 4, transcendentals=rows
        ),
        name="normalise",
    )(table, tokens, norm_gain.reshape(1, width))


def project_body(left_ref, *refs):
    parts, out_ref, right_ref = refs[:-2], refs[-2], refs[-1]
    at = 0
    for part_ref in parts:
        depth = part_ref.shape[0]
        right_ref[at : at + depth, :] = part_ref[...]
        at += depth
    out_ref[...] = jnp.dot(left_ref[...], right_ref[...], preferred_element_type=jnp.float32)


def projected(left, parts):
    rows, depth = left.shape
    columns = parts[0].shape[1]
    tile = min(columns, 256)
    if any(part.shape[0] % LANES for part in parts):
        return jnp.dot(left, jnp.concatenate(parts, axis=0), preferred_element_type=jnp.float32)
    return pl.pallas_call(
        project_body,
        grid=(columns // tile,),
        in_specs=[pl.BlockSpec((rows, depth), lambda j: (0, 0))]
        + [pl.BlockSpec((part.shape[0], tile), lambda j: (0, j)) for part in parts],
        out_specs=pl.BlockSpec((rows, tile), lambda j: (0, j)),
        out_shape=jax.ShapeDtypeStruct((rows, columns), jnp.float32),
        scratch_shapes=[pltpu.VMEM((depth, tile), jnp.bfloat16)],
        cost_estimate=pl.CostEstimate(
            flops=2 * rows * depth * columns,
            bytes_accessed=2 * depth * (rows + columns) + 4 * rows * columns,
            transcendentals=0,
        ),
        name="project",
    )(left, *parts)


def place_body(turn, here_ref, back_ref, cosine_ref, sine_ref, onehot_ref, *out_refs):
    rows = here_ref[...] + back_ref[...]
    if turn:
        is_key = pl.program_id(0) * rows.shape[1] < turn
        heads = []
        for at in range(0, rows.shape[1], HEAD):
            head = rows[:, at : at + HEAD]
            flipped = pltpu.roll(head, HEAD // 2, 1)
            turned = head * cosine_ref[...] + flipped * sine_ref[...]
            heads.append(jnp.where(is_key, turned, head))
        rows = jnp.concatenate(heads, axis=1)
    rows = rows.astype(jnp.bfloat16)
    region = CAP * PAGE
    placed = jnp.dot(onehot_ref[...], rows, preferred_element_type=jnp.float32)
    for k, out_ref in enumerate(out_refs):
        out_ref[...] = placed[k * region : (k + 1) * region].astype(jnp.bfloat16)


def placed_regions(turn, here, back, cosine, sine, onehot):
    rows, columns = here.shape
    tile = min(columns, 256)
    regions = 2 * REACH + 1
    region = CAP * PAGE
    column_block = pl.BlockSpec((rows, tile), lambda j: (0, j))
    whole = lambda array: pl.BlockSpec(array.shape, lambda j: (0, 0))
    return pl.pallas_call(
        functools.partial(place_body, turn),
        grid=(columns // tile,),
        in_specs=[column_block, column_block, whole(cosine), whole(sine), whole(onehot)],
        out_specs=[pl.BlockSpec((region, tile), lambda j: (0, j))] * regions,
        out_shape=[jax.ShapeDtypeStruct((region, columns), jnp.bfloat16)] * regions,
        cost_estimate=pl.CostEstimate(
            flops=2 * rows * SLOTS * PAGE * columns,
            bytes_accessed=8 * rows * columns,
            transcendentals=0,
        ),
        name="place",
    )(here, back, cosine, sine, onehot)


def handed_over(regions):
    arrived = []
    for k, region in enumerate(regions):
        arrived.append(region if k == REACH else shifted(region, "seq", k - REACH))
    return jnp.concatenate(arrived, axis=0)


def on_device(tokens, norm_gain, w_key, w_value, lengths, page_table):
    axis_size = lax.axis_size("seq")
    groups = lax.axis_size("group")
    device_index = lax.axis_index("seq")
    core = device_index % CORES
    tok_rows, width = tokens.shape
    part = width // axis_size // groups

    turns = [w_key.shape[1], 0]
    pieces = [opened(shard) for shard in (w_key, w_value)]

    order = arrival_order()
    table = jnp.stack(
        [
            jnp.stack([(place * CORES + which) * groups + owner for place, owner in order])
            for which in (core, CORES - 1 - core)
        ]
    ).astype(jnp.int32)
    mine, other = normalised(tokens, norm_gain, table, part)
    theirs = swapped(other, "seq")

    length_each = tok_rows * axis_size // 2
    token_index = device_index * tok_rows + jnp.arange(tok_rows, dtype=jnp.int32)
    prompt_id = token_index // length_each
    position = token_index % length_each
    limit = jnp.where(prompt_id == 0, lengths[0], lengths[1])
    inside = position < limit
    half = HEAD // 2
    freq = ROPE_THETA ** (-(jnp.arange(half, dtype=jnp.float32) * 2.0 / HEAD))
    angle = position.astype(jnp.float32)[:, None] * freq[None, :]
    cosine = jnp.cos(angle)
    sine = jnp.sin(angle)
    cosine = jnp.concatenate([cosine, cosine], axis=1)
    sine = jnp.concatenate([-sine, sine], axis=1)

    local_slot = page_table % SLOTS
    token_slot = (
        jnp.repeat(local_slot, PAGE) * PAGE + jnp.arange(tok_rows, dtype=jnp.int32) % PAGE
    )
    token_slot = jnp.where(inside, token_slot, -1)
    onehot = (
        jnp.arange(SLOTS * PAGE, dtype=jnp.int32)[:, None] == token_slot[None, :]
    ).astype(jnp.bfloat16)

    arrived = []
    for index, (whole, far, rest) in enumerate(pieces):
        parts = exchanged(whole, far, crossed(rest))
        there = projected(theirs, parts)
        back = swapped(there, "seq")
        here = projected(mine, parts)
        regions = placed_regions(turns[index], here, back, cosine, sine, onehot)
        arrived.append(handed_over(regions))
    keys, values = arrived
    return jnp.stack([keys, values]).reshape(2, SLOTS, PAGE, keys.shape[1])


def solution(mesh):
    placed = (
        P(("group", "seq"), None),
        P(),
        P("seq", None),
        P("seq", None),
        P("group"),
        P(("group", "seq")),
    )
    return jax.shard_map(
        on_device,
        mesh=mesh,
        in_specs=placed,
        out_specs=P(None, ("group", "seq"), None, None),
        check_vma=False,
    )
```
